32 devices in a mesh: order: 8 (over y, x, core), axial: 4 (over z).
Axes of the slice: x: 2, y: 2, z: 4, core: 2. Of those that a mesh axis runs over, the one named last changes fastest.
Arguments:
- coefficients: bfloat16 [4, 2, 1024, 8, 1024], P(None, None, 'order', 'axial'), may hold values from -0.005859375 to 0.005859375
- order_lists: int32 [1024], replicated, may hold values from 0 to 1023, as said below
- lengths: int32 [1024], replicated, may hold values from 128 to 1024, as said below
Outputs:
- advection: bfloat16 [3, 2, 1024, 8, 1024], P(None, None, 'order', 'axial')
The draws below stay inside these ranges and needn't reach their ends.
Inputs may be any that keep to these rules, and one draw needn't show every extreme that they name: `order_lists`: a permutation of the orders 0 to 1023; the device with index j along order holds slots j * 128 to (j + 1) * 128 - 1 of coefficients and advection. lengths[m] minus (128 + ((1023 - m) * 768) // 1023) lies in 0 to 128.
All inputs are finite; a program needn't handle non-finite values.
Results may differ from the reference program's by a relative error of at most 0.0095.
Values may be sent and summed in bfloat16 or wider, within the bound.
A program may use at most 128 MiB of HBM per device.

```python
import math
import jax
import jax.numpy as jnp
from jax import lax

M = 1024
R = 1024
K = 1024
NA = 2048
NZ = 8
MO = 128


def draw_order_lists(key, part):
    key_spread, key_blocks, key_shuffle = jax.random.split(jax.random.fold_in(key, 11), 3)
    group_count = M // MO
    position = jnp.arange(M, dtype=jnp.int32)
    spread = jax.random.randint(key_spread, (M,), 0, 4 * MO, dtype=jnp.int32)
    dealt_ids = jnp.argsort((position + spread) * M + position, stable=True).astype(jnp.int32)
    blocks = dealt_ids.reshape(group_count, MO)
    blocks = jnp.take(blocks, jax.random.permutation(key_blocks, group_count), axis=0)
    shuffle = jax.random.randint(key_shuffle, (group_count, MO), 0, M, dtype=jnp.int32)
    inside = jnp.argsort(shuffle * MO + jnp.arange(MO, dtype=jnp.int32)[None, :], axis=1, stable=True)
    blocks = jnp.take_along_axis(blocks, inside, axis=1)
    return blocks.reshape(M).astype(jnp.int32)


def draw_lengths(key, part):
    position = jnp.arange(M, dtype=jnp.int32)
    jitter = jax.random.randint(jax.random.fold_in(key, 23), (M,), 0, K // 8 + 1, dtype=jnp.int32)
    jitter = jnp.where(position == 0, K // 8, jnp.where(position == M - 1, 0, jitter))
    trend = K // 8 + (M - 1 - position) * (K - K // 4) // (M - 1)
    return (trend + jitter).astype(jnp.int32)


def steps_of(key, extent, shards, least, largest):
    def one(dim, parts):
        heights = jax.random.uniform(jax.random.fold_in(jax.random.fold_in(key, 6), dim), (parts,), jnp.float32, least / len(shards), largest / len(shards))
        return jnp.repeat(jnp.exp(heights), extent[dim] // parts).reshape((-1,) + (1,) * (len(extent) - dim - 1))

    loudness = one(*shards[0])
    for cut in shards[1:]:
        loudness = loudness * one(*cut)
    return loudness


def normal_values(key, shape, deviation, bound, cuts=(), kind=jnp.bfloat16):
    drawn = deviation * jax.random.normal(key, shape, jnp.float32)
    if cuts:
        drawn = drawn * steps_of(key, shape, cuts, -0.22, 0.18)
    return jnp.clip(drawn, -bound, bound).astype(kind)


def setup_inputs(seed: int = 0) -> dict:
    key_list = jax.random.split(jax.random.key(seed), 4)
    return {
        "coefficients": normal_values(key_list[0], (4, 2, M, NZ, K), (M * K) ** -0.5, 0.005859375, ((2, 8), (3, 4))),
        "order_lists": draw_order_lists(jax.random.fold_in(key_list[3], 71), 0),
        "lengths": draw_lengths(jax.random.fold_in(key_list[3], 71), 0),
    }


def radial_tables(radius_count, mode_count):
    radius_ids = jnp.arange(radius_count, dtype=jnp.int32)
    mode_ids = jnp.arange(mode_count, dtype=jnp.int32)
    phases = mode_ids[None, :] * (2 * radius_ids[:, None] + 1) % (4 * radius_count)
    angles_rad = phases.astype(jnp.float32) * (math.pi / (2 * radius_count))
    synthesis = jnp.cos(angles_rad).astype(jnp.bfloat16)
    analysis = (jnp.cos(angles_rad.T) * math.sqrt(2.0 / radius_count)).astype(jnp.bfloat16)
    return (synthesis, analysis)

def azimuthal_tables(order_ids, point_count):
    points = jnp.arange(point_count, dtype=jnp.int32)
    phases = order_ids[..., None] * points % point_count
    angles_rad = phases.astype(jnp.float32) * (2.0 * math.pi / point_count)
    cosines = jnp.cos(angles_rad)
    sines = jnp.sin(angles_rad)
    weight = jnp.where(order_ids == 0, 1.0, 2.0).astype(jnp.float32)[..., None]
    forward = jnp.stack((weight * cosines, -weight * sines), axis=-3).astype(jnp.bfloat16)
    factor = math.sqrt(2.0 / point_count)
    inverse = jnp.stack((cosines * factor, -sines * factor), axis=-3).astype(jnp.bfloat16)
    return (forward, inverse)

def reference(coefficients, order_lists, lengths):
    synthesis, analysis = radial_tables(R, K)
    forward, inverse = azimuthal_tables(order_lists, NA)
    synthesis_f = synthesis.astype(jnp.float32)
    analysis_f = analysis.astype(jnp.float32)
    forward_f = forward.astype(jnp.float32)
    inverse_f = inverse.astype(jnp.float32)
    slot_lengths = jnp.take(lengths, order_lists.astype(jnp.int32))
    retained = jnp.arange(K, dtype=jnp.int32)[None, :] < slot_lengths[:, None]
    plane_major = jnp.moveaxis(coefficients, 3, 0)

    def to_physical(plane_in):
        masked = jnp.where(retained[None, None], plane_in, 0).astype(jnp.float32)
        radial = jnp.einsum('fcmk,rk->fcmr', masked, synthesis_f).astype(jnp.bfloat16)
        physical = jnp.einsum('fcmr,cmj->frj', radial.astype(jnp.float32), forward_f)
        return physical.astype(jnp.bfloat16)
    physical = lax.map(to_physical, plane_major)
    plane_total = physical.shape[0]

    def advect(position):

        def plane_at(offset):
            where_at = ((position + offset) % plane_total).astype(jnp.int32)
            return lax.dynamic_index_in_dim(physical, where_at, 0, keepdims=False).astype(jnp.float32)
        current = plane_at(0)
        ahead_one = plane_at(1)
        behind_one = plane_at(-1)
        ahead_two = plane_at(2)
        behind_two = plane_at(-2)
        gradient = (8.0 * (ahead_one[:3] - behind_one[:3]) - (ahead_two[:3] - behind_two[:3])) / 12.0
        products = (current[3][None] * gradient).astype(jnp.bfloat16)
        spectral = jnp.einsum('grj,cmj->gcmr', products.astype(jnp.float32), inverse_f).astype(jnp.bfloat16)
        result = jnp.einsum('gcmr,kr->gcmk', spectral.astype(jnp.float32), analysis_f)
        return jnp.where(retained[None, None], result, 0.0).astype(jnp.bfloat16)
    advected = lax.map(advect, jnp.arange(plane_total, dtype=jnp.int32))
    return jnp.moveaxis(advected, 0, 3)
```

```python
import functools
import math

import jax
import jax.numpy as jnp
from jax import lax
from jax.experimental import pallas as pl
from jax.experimental.pallas import tpu as pltpu
from jax.sharding import PartitionSpec as P


R = 1024


def table_kernel(ca, sa, cb, sb, out):
    width = cb.shape[1]
    for h in range(ca.shape[1]):
        c0, s0 = ca[:, h : h + 1], sa[:, h : h + 1]
        cols = slice(h * width, (h + 1) * width)
        out[0, 0, :, cols] = (c0 * cb[...] - s0 * sb[...]).astype(out.dtype)
        if out.shape[1] > 1:
            out[0, 1, :, cols] = (-s0 * cb[...] - c0 * sb[...]).astype(out.dtype)


def wave_table(ids, groups, period, columns, kinds):
    count = ids.shape[0]
    rows = count // groups
    low = 128
    high = columns // low

    def parts(steps):
        angle = ((ids[:, None] * steps[None, :]) % period).astype(jnp.float32) * (
            2.0 * math.pi / period
        )
        return jnp.cos(angle), jnp.sin(angle)

    ca, sa = parts(jnp.arange(high, dtype=jnp.int32) * low)
    cb, sb = parts(jnp.arange(low, dtype=jnp.int32))
    spec_a = pl.BlockSpec((rows, high), lambda i: (i, 0))
    spec_b = pl.BlockSpec((rows, low), lambda i: (i, 0))
    return pl.pallas_call(
        table_kernel,
        grid=(groups,),
        in_specs=[spec_a, spec_a, spec_b, spec_b],
        out_specs=pl.BlockSpec((1, kinds, rows, columns), lambda i: (i, 0, 0, 0)),
        out_shape=jax.ShapeDtypeStruct((groups, kinds, rows, columns), jnp.bfloat16),
        cost_estimate=pl.CostEstimate(
            flops=6 * kinds * count * columns,
            bytes_accessed=2 * kinds * count * columns,
            transcendentals=0,
        ),
        name="wave_table",
    )(ca, sa, cb, sb).reshape(kinds * count, columns)


def gather_rows(x, xs, planes):
    groups, band, width = x.shape
    part = width // planes
    for i in range(groups):
        for z in range(planes):
            xs[z * band : (z + 1) * band, i * part : (i + 1) * part] = x[
                i, :, z * part : (z + 1) * part
            ]


def physical_kernel(planes, x, table, out, xs):
    @pl.when(pl.program_id(0) == 0)
    def _():
        gather_rows(x, xs, planes)

    out[...] = jnp.dot(xs[...], table[...], preferred_element_type=jnp.float32).astype(out.dtype)


def product_kernel(planes, factor, x, table, advecting, out, xs, total):
    step = pl.program_id(0)

    @pl.when(step == 0)
    def _():
        gather_rows(x, xs, planes)

    gradient = jnp.dot(xs[...], table[...], preferred_element_type=jnp.float32)
    products = (advecting[...].astype(jnp.float32) * gradient).astype(jnp.bfloat16)
    term = lax.dot_general(
        products, table[...], (((1,), (1,)), ((), ())), preferred_element_type=jnp.float32
    )

    @pl.when(step == 0)
    def _():
        total[...] = term

    @pl.when(step > 0)
    def _():
        total[...] += term

    @pl.when(step == pl.num_programs(0) - 1)
    def _():
        groups, band, width = out.shape
        part = width // planes
        for i in range(groups):
            for z in range(planes):
                out[i, :, z * part : (z + 1) * part] = (
                    total[z * band : (z + 1) * band, i * part : (i + 1) * part] * factor
                ).astype(out.dtype)


def call_physical(x, table, planes):
    groups, band, width = x.shape
    rows, depth, points = planes * band, table.shape[0], table.shape[1]
    tile = min(512, points)
    return pl.pallas_call(
        functools.partial(physical_kernel, planes),
        grid=(points // tile,),
        in_specs=[
            pl.BlockSpec((groups, band, width), lambda j: (0, 0, 0)),
            pl.BlockSpec((depth, tile), lambda j: (0, j)),
        ],
        out_specs=pl.BlockSpec((rows, tile), lambda j: (0, j)),
        out_shape=jax.ShapeDtypeStruct((rows, points), jnp.bfloat16),
        scratch_shapes=[pltpu.VMEM((rows, depth), jnp.bfloat16)],
        cost_estimate=pl.CostEstimate(
            flops=2 * rows * depth * points, bytes_accessed=2 * depth * points, transcendentals=0
        ),
        name="physical",
    )(x, table)


def call_products(x, table, advecting, planes, factor):
    groups, band, width = x.shape
    rows, depth, points = planes * band, table.shape[0], table.shape[1]
    tile = min(512, points)
    whole = pl.BlockSpec((groups, band, width), lambda j: (0, 0, 0))
    return pl.pallas_call(
        functools.partial(product_kernel, planes, factor),
        grid=(points // tile,),
        in_specs=[
            whole,
            pl.BlockSpec((depth, tile), lambda j: (0, j)),
            pl.BlockSpec((rows, tile), lambda j: (0, j)),
        ],
        out_specs=whole,
        out_shape=jax.ShapeDtypeStruct(x.shape, jnp.bfloat16),
        scratch_shapes=[
            pltpu.VMEM((rows, depth), jnp.bfloat16),
            pltpu.VMEM((rows, depth), jnp.float32),
        ],
        cost_estimate=pl.CostEstimate(
            flops=4 * rows * depth * points, bytes_accessed=2 * depth * points, transcendentals=0
        ),
        name="products",
    )(x, table, advecting)


def split_kernel(source, _, out):
    for c in range(out.shape[1]):
        value = source[0, c].astype(jnp.float32)
        for z in range(out.shape[0]):
            out[z, c] = value[:, z, :].astype(out.dtype)


def call_split(coefficients, field, after):
    _, parts, slots, planes, modes = coefficients.shape
    tile = min(256, modes)
    return pl.pallas_call(
        split_kernel,
        grid=(modes // tile,),
        in_specs=[
            pl.BlockSpec((1, parts, slots, planes, tile), lambda k: (field, 0, 0, 0, k)),
            pl.BlockSpec(memory_space=pl.ANY),
        ],
        out_specs=pl.BlockSpec((planes, parts, slots, tile), lambda k: (0, 0, 0, k)),
        out_shape=jax.ShapeDtypeStruct((planes, parts, slots, modes), coefficients.dtype),
        cost_estimate=pl.CostEstimate(
            flops=0, bytes_accessed=4 * parts * slots * planes * modes, transcendentals=0
        ),
        name="split",
    )(coefficients, after)


def radial_kernel(width, *refs):
    *sources, scale, synthesis, _, out = refs
    planes, parts, slots, _ = sources[0].shape if len(sources) == 1 else sources[1].shape
    groups, band, _ = out.shape

    def plane(z, c):
        if len(sources) == 1:
            return sources[0][z, c].astype(jnp.float32)
        low, own, high = sources
        if z < width:
            return low[z, c].astype(jnp.float32)
        if z < width + planes:
            return own[z - width, c].astype(jnp.float32)
        return high[z - width - planes, c].astype(jnp.float32)

    for z in range(planes):
        for c in range(parts):
            if len(sources) == 1:
                value = plane(z, c)
            else:
                value = (
                    8.0 * (plane(z + 3, c) - plane(z + 1, c)) - (plane(z + 4, c) - plane(z, c))
                ) / 12.0
            rows = (value * scale[...]).astype(jnp.bfloat16)
            first = (z * parts + c) * slots
            for i in range(groups):
                out[i, :, first : first + slots] = lax.dot_general(
                    synthesis[i * band : (i + 1) * band],
                    rows,
                    (((1,), (1,)), ((), ())),
                    preferred_element_type=jnp.float32,
                ).astype(out.dtype)


def call_radial(sources, scale, synthesis, after, groups, width):
    planes, parts, slots, modes = sources[len(sources) // 2].shape
    radii = synthesis.shape[0]
    columns = planes * parts * slots
    held = pl.BlockSpec(memory_space=pltpu.VMEM)
    return pl.pallas_call(
        functools.partial(radial_kernel, width),
        in_specs=[held] * (len(sources) + 2) + [pl.BlockSpec(memory_space=pl.ANY)],
        out_specs=held,
        out_shape=jax.ShapeDtypeStruct((groups, radii // groups, columns), jnp.bfloat16),
        cost_estimate=pl.CostEstimate(
            flops=2 * radii * columns * modes, bytes_accessed=8 * columns * modes, transcendentals=0
        ),
        name="radial",
    )(*sources, scale, synthesis, after)


def analysis_kernel(y, synthesis, kept, *refs):
    out = refs[-1]
    _, parts, slots, planes, _ = out.shape
    held = y[...].reshape(synthesis.shape[0], -1)
    for c in range(parts):
        rows = []
        for z in range(planes):
            first = (z * parts + c) * slots
            term = lax.dot_general(
                held[:, first : first + slots],
                synthesis[...],
                (((0,), (0,)), ((), ())),
                preferred_element_type=jnp.float32,
            )
            rows.append(term * kept[...])
        out[0, c] = jnp.stack(rows, axis=1).astype(out.dtype)


def call_analysis(y, synthesis, kept, field, shape, so_far):
    _, modes = synthesis.shape
    held = pl.BlockSpec(memory_space=pltpu.VMEM)
    more = () if so_far is None else (so_far,)
    return pl.pallas_call(
        analysis_kernel,
        grid=(1,),
        in_specs=[
            pl.BlockSpec(y.shape, lambda i: (0, 0, 0)),
            pl.BlockSpec(synthesis.shape, lambda i: (0, 0)),
            pl.BlockSpec(kept.shape, lambda i: (0, 0)),
        ]
        + [pl.BlockSpec(memory_space=pl.ANY)] * len(more),
        out_specs=pl.BlockSpec((1,) + shape[1:], lambda i: (field, 0, 0, 0, 0)),
        out_shape=jax.ShapeDtypeStruct(shape, jnp.bfloat16),
        input_output_aliases={3: 0} if more else {},
        cost_estimate=pl.CostEstimate(
            flops=2 * y.size * modes, bytes_accessed=4 * y.size, transcendentals=0
        ),
        name="analysis",
    )(y, synthesis, kept, *more)


def shards(coefficients, order_lists, lengths):
    field_count, part_count, slots, planes, modes = coefficients.shape
    order_count = order_lists.shape[0]
    points = 2 * order_count
    groups = lax.axis_size("order")
    axial = lax.axis_size("axial")
    width = 2
    onward = [(i, (i + 1) % axial) for i in range(axial)]
    backward = [(b, a) for a, b in onward]

    owns, halos = [], []
    after = order_lists
    for f in range(field_count):
        owns.append(call_split(coefficients, f, after))
        after = owns[f]
    for g in range(3):
        low = lax.ppermute(owns[g][planes - width :], "axial", onward)
        high = lax.ppermute(owns[g][:width], "axial", backward)
        halos.append((low, high))

    radius_ids = jnp.arange(R, dtype=jnp.int32)
    mode_ids = jnp.arange(modes, dtype=jnp.int32)
    synthesis = wave_table(2 * radius_ids + 1, groups, 4 * R, modes, 1)

    owned = lax.dynamic_slice_in_dim(order_lists, lax.axis_index("order") * slots, slots)
    catalog = jnp.arange(order_count, dtype=jnp.int32)
    own_lengths = jnp.sum(
        jnp.where(owned[:, None] == catalog[None, :], lengths[None, :], 0), axis=1
    )
    retained = mode_ids[None, :] < own_lengths[:, None]
    weight = jnp.where(owned == 0, 1.0, 2.0).astype(jnp.float32)[:, None]
    scale = jnp.where(retained, weight, 0.0)
    table = wave_table(order_lists, groups, points, points, 2)

    def exchange(x):
        return lax.all_to_all(x, "order", split_axis=0, concat_axis=0, tiled=True)

    first = call_radial((owns[3],), scale, synthesis, order_lists, groups, width)
    carried = exchange(first)
    advecting = call_physical(carried, table, planes)

    kept = jnp.where(retained, math.sqrt(2.0 / R), 0.0).astype(jnp.float32)
    after, result = carried, None
    for g in range(3):
        low, high = halos[g]
        radial = call_radial((low, owns[g], high), scale, synthesis, after, groups, width)
        arrived = exchange(radial)
        after = advecting if g == 0 else arrived
        products = call_products(
            arrived, table, advecting, planes, math.sqrt(2.0 / points)
        )
        spectral = exchange(products)
        shape = (3, part_count, slots, planes, modes)
        result = call_analysis(spectral, synthesis, kept, g, shape, result)
    return result


def solution(mesh):
    placed = (P(None, None, "order", "axial", None), P(), P())
    return jax.shard_map(
        shards,
        mesh=mesh,
        in_specs=placed,
        out_specs=P(None, None, "order", "axial", None),
        check_vma=False,
    )
```
